32 devices in a mesh: seq: 8 (over z, y), head: 4 (over x, core).
Axes of the slice: x: 2, y: 2, z: 4, core: 2. Of those that a mesh axis runs over, the one named last changes fastest.
Arguments:
- inputs: float32 [1024, 1024], P('seq', 'head'), may hold values from -6 to 6
- proj_weights: float32 [1024, 3, 512], P(None, None, 'head'), may hold values from -0.1875 to 0.1875
- out_grads: float32 [1024, 512], P('seq', 'head'), may hold values from -6 to 6
Outputs:
- grad_inputs: float32 [1024, 1024], P('seq', 'head')
- grad_weights: float32 [1024, 3, 512], P('seq', None, 'head')
The draws below stay inside these ranges and needn't reach their ends.
All inputs are finite; a program needn't handle non-finite values.
Results may differ from the reference program's by a relative error of at most 0.0003.
Values sent between devices are 32-bit elements; how exact they have to be, the bound alone decides.
No kernel may reach another device: no remote copies, remote signals or barrier semaphores. Data moves between devices by JAX's collectives and lax.ppermute only.
A program may use at most 128 MiB of HBM per device.

```python
import jax
import jax.numpy as jnp
import numpy as np
from jax import lax

D = 1024
HEADS = 8
HEAD_DIM = 64
T_DEV = 128
TOKENS = 1024


def steps_of(own_key, extent, shards, low, top_value):
    loudness, own = 1.0, jax.random.fold_in(own_key, 6)
    for position, parts in shards:
        heights = jnp.exp(jax.random.uniform(jax.random.fold_in(own, position), (parts,), jnp.float32, low / len(shards), top_value / len(shards)))
        loudness = loudness * jnp.repeat(heights, extent[position] // parts).reshape([-1 if axis == position else 1 for axis in range(len(extent))])
    return loudness


def scatter_about(key, extent, scale, bound, shards=(), held_as=jnp.bfloat16):
    result = scale * jax.random.normal(key, extent, jnp.float32)
    if shards:
        result = result * steps_of(key, extent, shards, -0.22, 0.18)
    return jnp.clip(result, -bound, bound).astype(held_as)


def setup_inputs(seed: int = 0) -> dict:
    key_of = jax.random.split(jax.random.key(seed), 4)
    inputs = scatter_about(key_of[0], (TOKENS, D), 1.0, 6.0, ((0, 8), (1, 4)), jnp.float32)
    proj_weights = scatter_about(key_of[1], (D, 3, HEADS * HEAD_DIM), D ** -0.5, 0.1875, ((2, 4),), jnp.float32)
    out_grads = scatter_about(key_of[2], (TOKENS, HEADS * HEAD_DIM), 1.0, 6.0, ((0, 8), (1, 4)), jnp.float32)
    return dict(inputs=inputs, proj_weights=proj_weights, out_grads=out_grads)


precise = lax.Precision.HIGHEST

def pair_tables(width):
    first_idx, second_idx = np.triu_indices(width)
    pair_scale = np.where(first_idx == second_idx, 1.0, np.sqrt(2.0))
    columns = np.arange(width)[:, None]
    table_one = jnp.asarray((columns == first_idx[None, :]) * pair_scale, jnp.float32)
    table_two = jnp.asarray((columns == second_idx[None, :]) * 1.0, jnp.float32)
    return (table_one, table_two)

def expand(vectors, table_one, table_two):
    part_one = jnp.einsum('hte,ef->htf', vectors, table_one, precision=precise)
    part_two = jnp.einsum('hte,ef->htf', vectors, table_two, precision=precise)
    return part_one * part_two

def forward(inputs, proj_weights):
    spans = TOKENS // T_DEV
    table_one, table_two = pair_tables(HEAD_DIM)
    pair_count = HEAD_DIM * (HEAD_DIM + 1) // 2

    def project(which_proj):
        flat = jnp.dot(inputs, proj_weights[:, which_proj, :], precision=precise)
        return flat.reshape(spans, T_DEV, HEADS, HEAD_DIM).transpose(0, 2, 1, 3)
    queries, keys_all, values = (project(0), project(1), project(2))
    causal = (jnp.arange(T_DEV)[:, None] >= jnp.arange(T_DEV)[None, :]).astype(jnp.float32)

    def span_step(carried, span_data):
        kv_state, kv_norms = carried
        query_blk, key_blk, value_blk = span_data
        query_feats = expand(query_blk, table_one, table_two) / HEAD_DIM
        key_feats = expand(key_blk, table_one, table_two)
        dots = jnp.einsum('hte,hse->hts', query_blk, key_blk, precision=precise)
        weights = dots * dots / HEAD_DIM * causal
        numerator = jnp.einsum('hts,hse->hte', weights, value_blk, precision=precise)
        numerator = numerator + jnp.einsum('htf,hfe->hte', query_feats, kv_state, precision=precise)
        denominator = 1.0 + lax.optimization_barrier(jnp.sum(weights, axis=-1)) + jnp.einsum('htf,hf->ht', query_feats, kv_norms, precision=precise)
        outputs = numerator / denominator[..., None]
        kv_state = kv_state + jnp.einsum('htf,hte->hfe', key_feats, value_blk, precision=precise)
        kv_norms = kv_norms + lax.optimization_barrier(jnp.sum(key_feats, axis=1))
        return ((kv_state, kv_norms), outputs)
    initial = (jnp.zeros((HEADS, pair_count, HEAD_DIM), jnp.float32), jnp.zeros((HEADS, pair_count), jnp.float32))
    _, outputs = lax.scan(jax.checkpoint(span_step), initial, (queries, keys_all, values))
    return outputs.transpose(0, 2, 1, 3).reshape(TOKENS, HEADS * HEAD_DIM)

def reference(inputs, proj_weights, out_grads):
    _, pullback = jax.vjp(forward, inputs, proj_weights)
    grad_inputs, grad_weights = pullback(out_grads)
    return (grad_inputs, grad_weights)
```

```python
import functools

import jax
import jax.numpy as jnp
import numpy as np
from jax import lax
from jax.experimental import pallas as pl
from jax.experimental.pallas import tpu as pltpu
from jax.sharding import PartitionSpec as P

HEAD_DIM = 64
LANES = 128
SPAN = 256
VMEM_BUDGET = 24 * 2**20

f32, bf16 = jnp.float32, jnp.bfloat16


precise = lax.Precision.HIGHEST


def pair_tables(width):
    first_idx, second_idx = np.triu_indices(width)
    pair_scale = np.where(first_idx == second_idx, 1.0, np.sqrt(2.0))
    columns = np.arange(width)[:, None]
    table_one = jnp.asarray((columns == first_idx[None, :]) * pair_scale, jnp.float32)
    table_two = jnp.asarray((columns == second_idx[None, :]) * 1.0, jnp.float32)
    return (table_one, table_two)


def expand_parts(vectors, tables):
    part_one = jnp.einsum("hte,ef->htf", vectors, tables[0], precision=precise)
    part_two = jnp.einsum("hte,ef->htf", vectors, tables[1], precision=precise)
    return (part_one, part_two)


def expand_grad(cotangent, parts, tables):
    first_term = jnp.einsum("htf,ef->hte", cotangent * parts[1], tables[0], precision=precise)
    second_term = jnp.einsum("htf,ef->hte", cotangent * parts[0], tables[1], precision=precise)
    return first_term + second_term


def flatten_rows(state_part, norm_part, groups):
    flat = jnp.concatenate([state_part.reshape(-1), norm_part.reshape(-1)])
    padded_len = -(-flat.shape[0] // groups) * groups
    flat = jnp.pad(flat, (0, padded_len - flat.shape[0]))
    return flat.reshape(groups, padded_len // groups)


def unflatten_rows(rows, state_part, norm_part):
    flat = rows.reshape(-1)
    state_size = state_part.size
    state_out = flat[:state_size].reshape(state_part.shape)
    norm_out = flat[state_size : state_size + norm_part.size].reshape(norm_part.shape)
    return (state_out, norm_out)


def earlier_sums(block):
    return jnp.cumsum(block, axis=0) - block


def later_sums(block):
    return jnp.sum(block, axis=0, keepdims=True) - jnp.cumsum(block, axis=0)


def key_prefix(state_part, norm_part):
    groups = lax.axis_size("seq")
    rows = flatten_rows(state_part, norm_part, groups)
    result = lax.all_to_all(
        earlier_sums(lax.all_to_all(rows, "seq", split_axis=0, concat_axis=0, tiled=True)),
        "seq",
        split_axis=0,
        concat_axis=0,
        tiled=True,
    )
    return unflatten_rows(result, state_part, norm_part)


def query_prefix(state_part, norm_part):
    groups = lax.axis_size("seq")
    rows = flatten_rows(state_part, norm_part, groups)
    result = lax.all_to_all(
        later_sums(lax.all_to_all(rows, "seq", split_axis=0, concat_axis=0, tiled=True)),
        "seq",
        split_axis=0,
        concat_axis=0,
        tiled=True,
    )
    return unflatten_rows(result, state_part, norm_part)


def per_device_states(inputs, proj_weights, out_grads):
    head_dim = HEAD_DIM
    pair_count = head_dim * (head_dim + 1) // 2
    local_width = proj_weights.shape[2]
    heads_here = local_width // head_dim
    tokens_here = inputs.shape[0]
    tables = pair_tables(head_dim)
    features = lax.all_gather(inputs, "head", axis=1, tiled=True)
    projected = jnp.einsum("td,dcf->ctf", features, proj_weights, precision=precise)

    def split_heads(matrix):
        return matrix.reshape(tokens_here, heads_here, head_dim).transpose(1, 0, 2)

    def merge_heads(tensor):
        return tensor.transpose(1, 0, 2).reshape(tokens_here, local_width)

    queries = split_heads(projected[0])
    keys_local = split_heads(projected[1])
    values = split_heads(projected[2])
    query_parts = expand_parts(queries, tables)
    key_parts = expand_parts(keys_local, tables)
    query_feats = query_parts[0] * query_parts[1] / head_dim
    key_feats = key_parts[0] * key_parts[1]
    state_local = jnp.einsum("htf,hte->fhe", key_feats, values, precision=precise).reshape(
        pair_count, local_width
    )
    norm_local = jnp.sum(key_feats, axis=1)
    state_prev, norm_prev = key_prefix(state_local, norm_local)
    state_heads = state_prev.reshape(pair_count, heads_here, head_dim)
    causal = (jnp.arange(tokens_here)[:, None] >= jnp.arange(tokens_here)[None, :]).astype(
        jnp.float32
    )
    dots = jnp.einsum("hte,hse->hts", queries, keys_local, precision=precise)
    weights = dots * dots / head_dim * causal
    numerator = jnp.einsum("hts,hse->hte", weights, values, precision=precise)
    numerator = numerator + jnp.einsum("htf,fhe->hte", query_feats, state_heads, precision=precise)
    denominator = (
        1.0
        + jnp.sum(weights, axis=-1)
        + jnp.einsum("htf,hf->ht", query_feats, norm_prev, precision=precise)
    )
    outputs = numerator / denominator[..., None]
    out_cot = split_heads(out_grads)
    grad_numer = out_cot / denominator[..., None]
    grad_denom = -jnp.sum(out_cot * outputs, axis=-1) / denominator
    grad_scores = (
        jnp.einsum("hte,hse->hts", grad_numer, values, precision=precise) + grad_denom[..., None]
    ) * causal
    grad_values = jnp.einsum("hts,hte->hse", weights, grad_numer, precision=precise)
    grad_dots = grad_scores * dots * (2.0 / head_dim)
    grad_queries = jnp.einsum("hts,hse->hte", grad_dots, keys_local, precision=precise)
    grad_keys = jnp.einsum("hts,hte->hse", grad_dots, queries, precision=precise)
    grad_qfeat = (
        jnp.einsum("hte,fhe->htf", grad_numer, state_heads, precision=precise)
        + grad_denom[..., None] * norm_prev[:, None, :]
    )
    adjoint_local = jnp.einsum("htf,hte->fhe", query_feats, grad_numer, precision=precise).reshape(
        pair_count, local_width
    )
    adjnorm_local = jnp.einsum("htf,ht->hf", query_feats, grad_denom, precision=precise)
    adjoint_next, adjnorm_next = query_prefix(adjoint_local, adjnorm_local)
    adjoint_heads = adjoint_next.reshape(pair_count, heads_here, head_dim)
    grad_kfeat = (
        jnp.einsum("hte,fhe->htf", values, adjoint_heads, precision=precise)
        + adjnorm_next[:, None, :]
    )
    grad_values = grad_values + jnp.einsum(
        "htf,fhe->hte", key_feats, adjoint_heads, precision=precise
    )
    grad_queries = grad_queries + expand_grad(grad_qfeat, query_parts, tables) / head_dim
    grad_keys = grad_keys + expand_grad(grad_kfeat, key_parts, tables)
    grad_proj = jnp.stack(
        [merge_heads(grad_queries), merge_heads(grad_keys), merge_heads(grad_values)], axis=0
    )
    input_terms = jnp.einsum("ctf,dcf->td", grad_proj, proj_weights, precision=precise)
    grad_inputs = lax.psum_scatter(input_terms, "head", scatter_dimension=1, tiled=True)
    rows_here = proj_weights.shape[0] // lax.axis_size("seq")
    weight_terms = jnp.einsum("td,ctf->dcf", features, grad_proj, precision=precise)
    totals = lax.psum(weight_terms, "seq")
    grad_weights = lax.dynamic_slice_in_dim(totals, lax.axis_index("seq") * rows_here, rows_here, 0)
    return (grad_inputs, grad_weights)


def dot(a, b, contract=((1,), (0,))):
    return lax.dot_general(a, b, (contract, ((), ())), preferred_element_type=f32)


NT = ((1,), (1,))


def split(x):
    hi = x.astype(bf16)
    return hi, (x - hi.astype(f32)).astype(bf16)


def vmem_call(kernel, out_shape, scratch, flops, args):
    spec = pl.BlockSpec(memory_space=pltpu.VMEM)
    bytes_moved = sum(a.size * a.dtype.itemsize for a in args)
    return pl.pallas_call(
        kernel,
        out_shape=out_shape,
        in_specs=[spec] * len(args),
        out_specs=jax.tree.map(lambda _: spec, out_shape),
        scratch_shapes=scratch,
        compiler_params=pltpu.CompilerParams(vmem_limit_bytes=40 * 2**20),
        cost_estimate=pl.CostEstimate(flops=flops, bytes_accessed=bytes_moved, transcendentals=0),
    )(*args)


def weights_kernel(w_ref, out_ref):
    for which in range(3):
        hi, lo = split(w_ref[which])
        out_ref[:, which * SPAN : which * SPAN + LANES] = hi
        out_ref[:, which * SPAN + LANES : (which + 1) * SPAN] = lo


def project_kernel(seq, *refs):
    x_refs, w_ref, out_ref, col_refs = refs[:4], refs[4], refs[5], refs[6:-2]
    lhs, columns = refs[-2:]
    rank, me = lax.axis_index("head"), lax.axis_index("seq")
    tokens, feats = x_refs[0].shape
    per_shard = feats // LANES
    for swap, ref in enumerate(x_refs):
        shard = lax.bitwise_xor(rank, jnp.int32(swap))
        hi, lo = split(ref[...])
        at = pl.ds(pl.multiple_of(shard * feats, feats), feats)
        lhs[:tokens, at] = hi
        lhs[tokens:, at] = lo
        for part in range(per_shard):
            columns[shard * per_shard + part] = ref[:, part * LANES : (part + 1) * LANES]
    for which in range(3):
        r = dot(lhs[...], w_ref[:, which * SPAN : (which + 1) * SPAN])
        r = r[:tokens] + r[tokens:]
        out = r[:, :LANES] + r[:, LANES:]
        out_ref[which * tokens : (which + 1) * tokens] = out * HEAD_DIM**-0.5 if which == 0 else out
    for step, col_ref in enumerate(col_refs):
        col_ref[...] = columns[lax.rem(me + step, seq)]


def block_ids(me, seq):
    lines = seq // 2
    line, side = me // 2, lax.rem(me, 2)
    at = [lax.rem(line + lines - k, lines) * 2 for k in range(lines)]
    return [a + side for a in at] + [a + 1 - side for a in at]


def pack(seq, qkv_refs, g_refs, dq, ck, dg, cv, cq, cg):
    tokens = g_refs[0].shape[0]
    low_lanes = lax.broadcasted_iota(jnp.int32, (tokens, LANES), 1) < HEAD_DIM
    for block, qkv, g in zip(block_ids(lax.axis_index("seq"), seq), qkv_refs, g_refs):
        rows = pl.ds(pl.multiple_of(block * tokens, tokens), tokens)
        values = [qkv[n * tokens : (n + 1) * tokens] for n in range(3)] + [g[...]]
        for n, x in enumerate(values):
            hi = x.astype(bf16).astype(f32)
            lo = x - hi
            hi_r, lo_r = pltpu.roll(hi, HEAD_DIM, 1), pltpu.roll(lo, HEAD_DIM, 1)
            both = [jnp.where(low_lanes, hi, lo_r), jnp.where(low_lanes, hi_r, lo)]
            his = [jnp.where(low_lanes, hi, hi_r), jnp.where(low_lanes, hi_r, hi)]
            los = [jnp.where(low_lanes, lo, lo_r), jnp.where(low_lanes, lo_r, lo)]
            for h in range(2):
                c = both[h].astype(bf16)
                if n in (1, 2):
                    ref = ck if n == 1 else cv
                    ref[h, rows, :LANES] = c
                    ref[h, rows, LANES:] = c
                else:
                    ref, small = (dq, cq) if n == 0 else (dg, cg)
                    ref[h, rows, :LANES] = his[h].astype(bf16)
                    ref[h, rows, LANES:] = los[h].astype(bf16)
                    small[h, rows] = c


def stack(x):
    hi, lo = split(x)
    return jnp.concatenate([hi, lo], axis=0)


def fold_lanes(r):
    half = r.shape[0] // 2
    r = r[:half] + r[half:]
    return r + pltpu.roll(r, HEAD_DIM, 1)


def own_kernel(seq, *refs):
    qkv_refs, g_refs = refs[:seq], refs[seq : 2 * seq]
    w_ref = refs[2 * seq]
    stat_ref, *part_refs = refs[2 * seq + 1 : 2 * seq + 6]
    dq, ck, dg, cv, cq, cg, sums, lhs = refs[2 * seq + 6 :]
    pack(seq, qkv_refs, g_refs, dq, ck, dg, cv, cq, cg)
    tokens = g_refs[0].shape[0]
    total = tokens * seq
    me, rank = lax.axis_index("seq"), lax.axis_index("head")
    spans = total // SPAN
    later = lax.broadcasted_iota(jnp.int32, (SPAN, SPAN), 1) >= lax.broadcasted_iota(jnp.int32, (SPAN, SPAN), 0)
    for h in range(2):
        for t in range(spans):
            t_rows = slice(t * SPAN, (t + 1) * SPAN)
            den = jnp.zeros((8, SPAN), f32)
            mix = jnp.zeros((8, SPAN), f32)
            for s in range(t + 1):
                s_rows = slice(s * SPAN, (s + 1) * SPAN)
                score = dot(ck[h, s_rows], dq[h, t_rows], NT)
                value = dot(cv[h, s_rows], dg[h, t_rows], NT)
                weight = score * score
                if s == t:
                    weight = jnp.where(later, weight, 0.0)
                den += jnp.sum(weight.reshape(SPAN // 8, 8, SPAN), axis=0)
                mix += jnp.sum((weight * value).reshape(SPAN // 8, 8, SPAN), axis=0)
            inv = 1.0 / (1.0 + jnp.sum(den, axis=0, keepdims=True))
            shift = -2.0 * inv * inv * jnp.sum(mix, axis=0, keepdims=True)
            stat_ref[h, 0:1, t_rows] = inv
            stat_ref[h, 1:2, t_rows] = 2.0 * inv
            stat_ref[h, 2:3, t_rows] = shift
    rows = pl.ds(pl.multiple_of(me * tokens, tokens), tokens)
    low_lanes = lax.broadcasted_iota(jnp.int32, (tokens, LANES), 1) < HEAD_DIM
    col = lax.broadcasted_iota(jnp.int32, (tokens, total), 1)
    row = lax.broadcasted_iota(jnp.int32, (tokens, total), 0) + me * tokens
    grads = []
    for h in range(2):
        score = dot(dq[h, rows], ck[h], NT)
        value = dot(dg[h, rows], cv[h], NT)
        scale = jnp.transpose(jnp.broadcast_to(stat_ref[h, 1:2, rows], (tokens, tokens)))[:, :1]
        shift = jnp.transpose(jnp.broadcast_to(stat_ref[h, 2:3, rows], (tokens, tokens)))[:, :1]
        adj = jnp.where(col <= row, score * (value * scale + shift), 0.0)
        d_q = fold_lanes(dot(stack(adj), ck[h, :, :LANES])) * HEAD_DIM**-0.5
        score = dot(ck[h, rows], dq[h], NT)
        value = dot(cv[h, rows], dg[h], NT)
        adj = jnp.where(col >= row, score * (value * stat_ref[h, 1:2] + stat_ref[h, 2:3]), 0.0)
        weight = jnp.where(col >= row, score * score * stat_ref[h, 0:1], 0.0)
        d_k = fold_lanes(dot(stack(adj), cq[h]))
        d_v = fold_lanes(dot(stack(weight), cg[h]))
        grads.append((d_q, d_k, d_v))
    for which in range(3):
        grad = jnp.where(low_lanes, grads[0][which], grads[1][which])
        hi, lo = split(grad)
        for half in range(2):
            at = which * SPAN + half * LANES
            lhs[:tokens, at : at + LANES] = hi
            lhs[tokens:, at : at + LANES] = lo
    feats = part_refs[0].shape[1]
    for swap in (3, 2, 1, 0):
        shard = lax.bitwise_xor(rank, jnp.int32(swap))
        r = dot(lhs[...], w_ref[pl.ds(pl.multiple_of(shard * feats, feats), feats)], NT)
        part_refs[swap][...] = r[:tokens] + r[tokens:]


def weight_grad_kernel(seq, *refs):
    qkv_refs, g_refs, col_refs = refs[:seq], refs[seq : 2 * seq], refs[2 * seq : 3 * seq]
    stat_ref, out_ref = refs[3 * seq : 3 * seq + 2]
    dq, ck, dg, cv, cq, cg, adj_hl, wgt_hl, grad, xs = refs[3 * seq + 2 :]
    pack(seq, qkv_refs, g_refs, dq, ck, dg, cv, cq, cg)
    tokens = g_refs[0].shape[0]
    total = tokens * seq
    me = lax.axis_index("seq")
    for step, ref in enumerate(col_refs):
        block = lax.rem(me + seq - step, seq)
        rows = pl.ds(pl.multiple_of(block * tokens, tokens), tokens)
        hi, lo = split(ref[...])
        xs[rows, :LANES] = hi
        xs[rows, LANES:] = lo
    spans = total // SPAN
    later = lax.broadcasted_iota(jnp.int32, (SPAN, SPAN), 1) >= lax.broadcasted_iota(jnp.int32, (SPAN, SPAN), 0)

    def halves(r):
        return r[:HEAD_DIM] + r[HEAD_DIM:]

    def times(c, hi, lo, contract):
        return halves(dot(c, hi, contract)) + dot(c[:HEAD_DIM], lo, contract)

    for h in range(2):
        q_t = jnp.transpose(cq[h].astype(f32)).astype(bf16)
        k_t = jnp.transpose(ck[h, :, :LANES].astype(f32)).astype(bf16)
        g_t = jnp.transpose(cg[h].astype(f32)).astype(bf16)
        for s in range(spans):
            s_rows = slice(s * SPAN, (s + 1) * SPAN)
            for t in range(s, spans):
                t_rows = slice(t * SPAN, (t + 1) * SPAN)
                score = dot(ck[h, s_rows], dq[h, t_rows], NT)
                value = dot(cv[h, s_rows], dg[h, t_rows], NT)
                if s == t:
                    score = jnp.where(later, score, 0.0)
                adj = score * (value * stat_ref[h, 1:2, t_rows] + stat_ref[h, 2:3, t_rows])
                weight = score * score * stat_ref[h, 0:1, t_rows]
                for hl, x in ((adj_hl, adj), (wgt_hl, weight)):
                    hi, lo = split(x)
                    hl[0, :, t_rows] = hi
                    hl[1, :, t_rows] = lo
            t_rows = slice(s * SPAN, total)
            q_at, k_at, v_at = (which * LANES + h * HEAD_DIM for which in range(3))
            d_q = times(k_t[:, s_rows], adj_hl[0, :, t_rows], adj_hl[1, :, t_rows], ((1,), (0,)))
            if s == 0:
                grad[q_at : q_at + HEAD_DIM] = d_q
            else:
                grad[q_at : q_at + HEAD_DIM, t_rows] += d_q
            grad[k_at : k_at + HEAD_DIM, s_rows] = times(q_t[:, t_rows], adj_hl[0, :, t_rows], adj_hl[1, :, t_rows], NT)
            grad[v_at : v_at + HEAD_DIM, s_rows] = times(g_t[:, t_rows], wgt_hl[0, :, t_rows], wgt_hl[1, :, t_rows], NT)
    for which in range(3):
        r = dot(stack(grad[which * LANES : (which + 1) * LANES]), xs[...])
        r = r[:LANES] + r[LANES:]
        r = jnp.transpose(r[:, :LANES] + r[:, LANES:])
        out_ref[which] = r * HEAD_DIM**-0.5 if which == 0 else r


def pairs(count, partner):
    return [(n, partner(n)) for n in range(count)]


def gather_seq(x, seq):
    lines = seq // 2
    own = [x] + [lax.ppermute(x, "seq", pairs(seq, lambda n: (n + 2 * k) % seq)) for k in range(1, lines)]
    return own + [lax.ppermute(b, "seq", pairs(seq, lambda n: n ^ 1)) for b in own]


def per_device_scores(inputs, proj_weights, out_grads):
    seq, heads = lax.axis_size("seq"), lax.axis_size("head")
    tokens, feats = inputs.shape
    depth, _, width = proj_weights.shape
    total = tokens * seq
    g_blocks = gather_seq(out_grads, seq)
    far = lax.ppermute(inputs, "head", pairs(heads, lambda n: n ^ 2))
    near = lax.ppermute(inputs, "head", pairs(heads, lambda n: n ^ 1))
    diagonal = lax.ppermute(far, "head", pairs(heads, lambda n: n ^ 1))
    shape = jax.ShapeDtypeStruct
    weights = vmem_call(
        weights_kernel,
        shape((depth, 3 * SPAN), bf16),
        [],
        depth * width * 3,
        (proj_weights.transpose(1, 0, 2),),
    )
    qkv, *columns = vmem_call(
        functools.partial(project_kernel, seq),
        [shape((3 * tokens, LANES), f32)] + [shape((tokens, LANES), f32)] * seq,
        [pltpu.VMEM((2 * tokens, depth), bf16), pltpu.VMEM((depth // LANES, tokens, LANES), f32)],
        2 * tokens * depth * width * 9,
        (inputs, near, far, diagonal, weights),
    )
    blocks = gather_seq(qkv, seq)
    columns = columns[:1] + [
        lax.ppermute(columns[k], "seq", pairs(seq, lambda n: (n + k) % seq)) for k in range(1, seq)
    ]
    packed = [pltpu.VMEM((2, total, SPAN), bf16)] * 4 + [pltpu.VMEM((2, total, LANES), bf16)] * 2
    stats, *parts = vmem_call(
        functools.partial(own_kernel, seq),
        [shape((2, 8, total), f32)] + [shape((tokens, feats), f32)] * heads,
        packed + [pltpu.VMEM((8, total), f32), pltpu.VMEM((2 * tokens, 3 * SPAN), bf16)],
        8 * total * total * SPAN,
        (*blocks, *g_blocks, weights),
    )
    received = [lax.ppermute(parts[k], "head", pairs(heads, lambda n: n ^ k)) for k in (3, 2, 1)]
    grad_weights = vmem_call(
        functools.partial(weight_grad_kernel, seq),
        shape((3, LANES, LANES), f32),
        packed
        + [pltpu.VMEM((2, SPAN, total), bf16)] * 2
        + [pltpu.VMEM((3 * LANES, total), f32), pltpu.VMEM((total, SPAN), bf16)],
        20 * total * total * SPAN,
        (*blocks, *g_blocks, *columns, stats),
    )
    grad_inputs = parts[0] + received[0] + received[1] + received[2]
    return (grad_inputs, grad_weights.transpose(1, 0, 2))


def per_device(inputs, proj_weights, out_grads):
    seq, heads = lax.axis_size("seq"), lax.axis_size("head")
    tokens, feats = inputs.shape
    depth, _, width = proj_weights.shape
    fits = tokens * seq * 12 * SPAN * 2 <= VMEM_BUDGET
    shaped = (
        heads == 4
        and seq % 2 == 0
        and tokens % LANES == 0
        and (tokens * seq) % SPAN == 0
        and width == LANES == 2 * HEAD_DIM
        and feats % LANES == 0
        and depth == seq * LANES
    )
    path = per_device_scores if fits and shaped else per_device_states
    return path(inputs, proj_weights, out_grads)


def solution(mesh):
    return jax.shard_map(
        per_device,
        mesh=mesh,
        in_specs=(P("seq", "head"), P(None, None, "head"), P("seq", "head")),
        out_specs=(P("seq", "head"), P("seq", None, "head")),
        check_vma=False,
    )
```
